32 devices in a mesh: cand: 4 (over y, core), feat: 8 (over z, x).
Axes of the slice: x: 2, y: 2, z: 4, core: 2. Of those that a mesh axis runs over, the one named last changes fastest.
Arguments:
- embeddings: bfloat16 [131072, 4096], P('cand', 'feat'), may hold values from -1 to 1
- winners: int32 [3], replicated, may hold values from 0 to 131071, as said below
Outputs:
- gains: float32 [131072], P('cand')
- coords: float32 [3, 131072], P(None, 'cand')
- best: float32 [3], replicated
The draws below stay inside these ranges and needn't reach their ends.
Inputs may be any that keep to these rules, and one draw needn't show every extreme that they name: `winners`: 3 different candidates.
All inputs are finite; a program needn't handle non-finite values.
Results may differ from the reference program's by a relative error of at most 0.0003.
Values may be sent and summed in bfloat16 or wider, within the bound.
No kernel may reach another device: no remote copies, remote signals or barrier semaphores. Data moves between devices by JAX's collectives and lax.ppermute only.
A program may use at most 128 MiB of HBM per device.

```python
import math
import jax
import jax.numpy as jnp
from jax import lax

D = 4096
STEPS = 3
CANDS = 131072


def draw_embeddings(key, part):
    keys = jax.random.split(jax.random.fold_in(key, 11), 5)
    noise = jnp.clip(jax.random.normal(keys[0], (CANDS, D), jnp.float32), -4.0, 4.0)
    shared = jax.random.uniform(keys[2], (CANDS, 1), jnp.float32, -1.0, 1.0)
    common = jnp.clip(jax.random.normal(keys[1], (1, D), jnp.float32), -4.0, 4.0)
    scales = jnp.exp(jax.random.uniform(keys[3], (CANDS, 1), jnp.float32, math.log(0.5), math.log(3.0)))
    rising = jnp.exp(math.log(3.0) * jnp.arange(D, dtype=jnp.float32) / D)[None, :]
    columns = rising * jax.random.uniform(keys[4], (1, D), jnp.float32, 0.7, 1.4)
    values = scales * columns * (noise + shared * common) / (1.8 * math.sqrt(D))
    return jnp.clip(values, -1.0, 1.0).astype(jnp.bfloat16)


def draw_winners(key, part):
    keys = jax.random.split(jax.random.fold_in(key, 23), 2)
    middle = jax.random.permutation(keys[0], CANDS - 2)[:STEPS - 2].astype(jnp.int32) + 1
    ends = jnp.array([0, CANDS - 1], dtype=jnp.int32)
    values = jnp.concatenate([ends, middle])
    order = jax.random.permutation(keys[1], STEPS)
    return values[order].astype(jnp.int32)


def setup_inputs(seed: int = 0) -> dict:
    streams_of = jax.random.split(jax.random.key(seed), 3)
    return {
        "embeddings": draw_embeddings(jax.random.fold_in(streams_of[2], 71), 0),
        "winners": draw_winners(jax.random.fold_in(streams_of[2], 71), 0),
    }


def reference(embeddings, winners):
    block = math.gcd(CANDS, 8192)
    blocks = embeddings.reshape(CANDS // block, block, D)
    norms = lax.map(lambda piece: lax.optimization_barrier(jnp.sum(jnp.square(piece.astype(jnp.float32)), axis=1)), blocks).reshape(CANDS)
    gains = norms
    coords = []
    best = []
    for step in range(STEPS):
        chosen = winners[step]
        row = lax.dynamic_index_in_dim(embeddings, chosen, 0, keepdims=False)
        dots = lax.map(lambda piece: jnp.dot(piece, row, preferred_element_type=jnp.float32), blocks).reshape(CANDS)
        proj = jnp.zeros((CANDS,), jnp.float32)
        for prior in range(step):
            proj = proj + coords[prior] * coords[prior][chosen]
        scale = jnp.sqrt(jnp.maximum(gains[chosen], 1.0))
        fresh = (dots - proj) / scale
        gains = gains - fresh * fresh
        coords.append(fresh)
        best.append(jnp.max(gains))
    return (gains, jnp.stack(coords), jnp.stack(best))
```

```python
import functools

import jax
import jax.numpy as jnp
from jax import lax
from jax.experimental import pallas as pl
from jax.experimental.pallas import tpu as pltpu
from jax.sharding import PartitionSpec as P

STEPS = 3
LANES = 128
SUB = 256
GROUP = 16
CALLS = 4
NT = (((1,), (1,)), ((), ()))


def pick_kernel(winner_ref, *refs, cand_rows):
    out_ref = refs[STEPS]
    out_ref[...] = jnp.zeros_like(out_ref)
    for step in range(STEPS):
        spot = lax.rem(lax.rem(winner_ref[step], cand_rows), GROUP)
        block = refs[step][...].astype(jnp.float32)
        keep = lax.broadcasted_iota(jnp.int32, block.shape, 0) == spot
        row = jnp.sum(jnp.where(keep, block, 0.0), axis=0, keepdims=True)
        out_ref[0, step : step + 1, :] = row.astype(jnp.bfloat16)


def pick(embeddings, winners):
    cand_rows, feats = embeddings.shape

    def spec(step):
        return pl.BlockSpec((GROUP, feats), lambda i, w: (lax.div(lax.rem(w[step], cand_rows), GROUP), 0))

    return pl.pallas_call(
        functools.partial(pick_kernel, cand_rows=cand_rows),
        grid_spec=pltpu.PrefetchScalarGridSpec(
            num_scalar_prefetch=1,
            grid=(1,),
            in_specs=[spec(step) for step in range(STEPS)],
            out_specs=pl.BlockSpec((1, 4, feats), lambda i, w: (0, 0, 0)),
        ),
        out_shape=jax.ShapeDtypeStruct((1, 4, feats), jnp.bfloat16),
        name="pick",
    )(winners, *([embeddings] * STEPS))


def scan_kernel(winner_ref, me_ref, picked_ref, emb_ref, out_ref, win_ref, *, rows, chunk, feats, cand_rows):
    part = pl.program_id(1)

    @pl.when((pl.program_id(0) == 0) & (part == 0))
    def _():
        win_ref[...] = jnp.zeros_like(win_ref)
        for step in range(STEPS):
            win_ref[step : step + 1, :] = picked_ref[lax.div(winner_ref[step], cand_rows), step : step + 1, :].astype(jnp.float32)

    wide = win_ref[...].astype(jnp.bfloat16)
    win = wide[0:8, :]

    @pl.when(part == 0)
    def _():
        gram = lax.dot_general(win, wide, NT, preferred_element_type=jnp.float32)
        out_ref[0, :, chunk : chunk + LANES] = gram[0:4, :]

    ones = (lax.broadcasted_iota(jnp.int32, (8, 2 * LANES), 0) == STEPS).astype(jnp.float32).astype(jnp.bfloat16)
    for sub in range(rows // SUB):
        block = emb_ref[sub * SUB : (sub + 1) * SUB, :]
        dots = lax.dot_general(win, block, NT, preferred_element_type=jnp.float32)
        total = None
        for lane in range(feats // LANES):
            piece = block[:, lane * LANES : (lane + 1) * LANES].astype(jnp.float32)
            total = piece * piece if total is None else total + piece * piece
        high = total.astype(jnp.bfloat16)
        low = (total - high.astype(jnp.float32)).astype(jnp.bfloat16)
        both = jnp.concatenate([high, low], axis=1)
        dots = dots + lax.dot_general(ones, both, NT, preferred_element_type=jnp.float32)
        start = pl.multiple_of(part * rows + sub * SUB, SUB)
        out_ref[0, :, pl.ds(start, SUB)] = dots[0:4, :]


def scan(embeddings, picked, winners, me, feat_size, first, count):
    cand_rows, feats = embeddings.shape
    chunk = cand_rows // feat_size
    rows = min(chunk, 2048)
    parts = chunk // rows
    return pl.pallas_call(
        functools.partial(scan_kernel, rows=rows, chunk=chunk, feats=feats, cand_rows=cand_rows),
        grid_spec=pltpu.PrefetchScalarGridSpec(
            num_scalar_prefetch=2,
            grid=(count, parts),
            in_specs=[
                pl.BlockSpec(picked.shape, lambda c, p, w, m: (0, 0, 0)),
                pl.BlockSpec((rows, feats), lambda c, p, w, m: (lax.bitwise_xor(m[0], first - c) * parts + p, 0)),
            ],
            out_specs=pl.BlockSpec((1, 4, chunk + LANES), lambda c, p, w, m: (c, 0, 0)),
            scratch_shapes=[pltpu.VMEM((LANES, feats), jnp.float32)],
        ),
        out_shape=jax.ShapeDtypeStruct((count, 4, chunk + LANES), jnp.float32),
        compiler_params=pltpu.CompilerParams(dimension_semantics=("arbitrary", "arbitrary")),
        name="scan",
    )(winners, me, picked, embeddings)


def update_kernel(*refs, feat_size, chunk):
    out_ref = refs[feat_size]
    total = refs[0][0]
    for src in range(1, feat_size):
        total = total + refs[src][0]
    table = total[:, chunk : chunk + LANES]
    gram = [[table[a : a + 1, b : b + 1] for b in range(STEPS)] for a in range(STEPS)]
    gains = total[STEPS : STEPS + 1, 0:chunk]
    coords = []
    winner_coords = [[None] * STEPS for _ in range(STEPS)]
    winner_gains = [gram[step][step] for step in range(STEPS)]
    for step in range(STEPS):
        scale = jnp.sqrt(jnp.maximum(winner_gains[step], 1.0))
        fresh = total[step : step + 1, 0:chunk]
        if step:
            proj = coords[0] * winner_coords[step][0]
            for prior in range(1, step):
                proj = proj + coords[prior] * winner_coords[step][prior]
            fresh = fresh - proj
        fresh = fresh / scale
        gains = gains - fresh * fresh
        coords.append(fresh)
        out_ref[step : step + 1, 0:chunk] = fresh
        out_ref[step : step + 1, chunk : chunk + LANES] = jnp.broadcast_to(jnp.max(gains, axis=1, keepdims=True), (1, LANES))
        for later in range(step + 1, STEPS):
            value = gram[later][step]
            for prior in range(step):
                value = value - winner_coords[later][prior] * winner_coords[step][prior]
            value = value / scale
            winner_coords[later][step] = value
            winner_gains[later] = winner_gains[later] - value * value
    out_ref[STEPS : STEPS + 1, 0:chunk] = gains
    out_ref[STEPS : STEPS + 1, chunk : chunk + LANES] = jnp.zeros((1, LANES), jnp.float32)


def update(parts, feat_size, chunk):
    return pl.pallas_call(
        functools.partial(update_kernel, feat_size=feat_size, chunk=chunk),
        out_shape=jax.ShapeDtypeStruct((4, chunk + LANES), jnp.float32),
        name="update",
    )(*parts)


def unpack_kernel(me_ref, *refs, feat_size, chunk):
    gains_ref, coords_ref, best_ref = refs[feat_size:]
    best = refs[0][:, chunk : chunk + LANES]
    for k in range(feat_size):
        start = pl.multiple_of(lax.bitwise_xor(me_ref[0], k) * chunk, chunk)
        coords_ref[:, pl.ds(start, chunk)] = refs[k][0:STEPS, 0:chunk]
        gains_ref[pl.ds(start, chunk)] = refs[k][STEPS : STEPS + 1, 0:chunk].reshape(chunk)
        best = jnp.maximum(best, refs[k][:, chunk : chunk + LANES])
    best_ref[...] = best


def unpack(pieces, me, feat_size, chunk):
    return pl.pallas_call(
        functools.partial(unpack_kernel, feat_size=feat_size, chunk=chunk),
        in_specs=[pl.BlockSpec(memory_space=pltpu.SMEM)] + [pl.BlockSpec(memory_space=pltpu.VMEM)] * feat_size,
        out_shape=(
            jax.ShapeDtypeStruct((feat_size * chunk,), jnp.float32),
            jax.ShapeDtypeStruct((STEPS, feat_size * chunk), jnp.float32),
            jax.ShapeDtypeStruct((4, LANES), jnp.float32),
        ),
        name="unpack",
    )(me, *pieces)


def swap(value, k, feat_size):
    return lax.ppermute(value, "feat", [(src, src ^ k) for src in range(feat_size)])


def per_device(embeddings, winners, *, feat_size):
    cand_rows = embeddings.shape[0]
    chunk = cand_rows // feat_size
    me = lax.axis_index("feat").astype(jnp.int32).reshape(1)
    picked = lax.all_gather(pick(embeddings, winners), "cand", axis=0, tiled=True)
    parts = []
    count = -(-feat_size // CALLS)
    first = feat_size - 1
    while first >= 0:
        here = min(count, first + 1)
        partial = scan(embeddings, picked, winners, me, feat_size, first, here)
        for c in range(here):
            piece = lax.slice_in_dim(partial, c, c + 1)
            k = first - c
            parts.append(swap(piece, k, feat_size) if k else piece)
        first -= here
    mine = update(parts, feat_size, chunk)
    pieces = [mine] + [swap(mine, k, feat_size) for k in range(1, feat_size)]
    gains, coords, best = unpack(pieces, me, feat_size, chunk)
    best = lax.pmax(best[0:STEPS, 0], "cand")
    return gains, coords, best


def solution(mesh):
    return jax.shard_map(
        functools.partial(per_device, feat_size=mesh.shape["feat"]),
        mesh=mesh,
        in_specs=(P("cand", "feat"), P()),
        out_specs=(P("cand"), P(None, "cand"), P()),
        check_vma=False,
    )
```

```python
import functools

import jax
import jax.numpy as jnp
from jax import lax
from jax.experimental import pallas as pl
from jax.experimental.pallas import tpu as pltpu
from jax.sharding import PartitionSpec as P

STEPS = 3
LANES = 128
SUB = 256
GROUP = 16
CALLS = 2
NT = (((1,), (1,)), ((), ()))


def pick_kernel(winner_ref, *refs, cand_rows):
    out_ref = refs[STEPS]
    out_ref[...] = jnp.zeros_like(out_ref)
    for step in range(STEPS):
        spot = lax.rem(lax.rem(winner_ref[step], cand_rows), GROUP)
        block = refs[step][...].astype(jnp.float32)
        keep = lax.broadcasted_iota(jnp.int32, block.shape, 0) == spot
        row = jnp.sum(jnp.where(keep, block, 0.0), axis=0, keepdims=True)
        out_ref[0, step : step + 1, :] = row.astype(jnp.bfloat16)


def pick(embeddings, winners):
    cand_rows, feats = embeddings.shape

    def spec(step):
        return pl.BlockSpec((GROUP, feats), lambda i, w: (lax.div(lax.rem(w[step], cand_rows), GROUP), 0))

    return pl.pallas_call(
        functools.partial(pick_kernel, cand_rows=cand_rows),
        grid_spec=pltpu.PrefetchScalarGridSpec(
            num_scalar_prefetch=1,
            grid=(1,),
            in_specs=[spec(step) for step in range(STEPS)],
            out_specs=pl.BlockSpec((1, 4, feats), lambda i, w: (0, 0, 0)),
        ),
        out_shape=jax.ShapeDtypeStruct((1, 4, feats), jnp.bfloat16),
        name="pick",
    )(winners, *([embeddings] * STEPS))


def scan_kernel(winner_ref, me_ref, picked_ref, emb_ref, out_ref, win_ref, *, rows, chunk, feats, cand_rows):
    part = pl.program_id(1)

    @pl.when((pl.program_id(0) == 0) & (part == 0))
    def _():
        win_ref[...] = jnp.zeros_like(win_ref)
        for step in range(STEPS):
            win_ref[step : step + 1, :] = picked_ref[lax.div(winner_ref[step], cand_rows), step : step + 1, :].astype(jnp.float32)

    wide = win_ref[...].astype(jnp.bfloat16)
    win = wide[0:8, :]

    @pl.when(part == 0)
    def _():
        gram = lax.dot_general(win, wide, NT, preferred_element_type=jnp.float32)
        out_ref[0, :, chunk : chunk + LANES] = gram[0:4, :]

    ones = (lax.broadcasted_iota(jnp.int32, (8, 2 * LANES), 0) == STEPS).astype(jnp.float32).astype(jnp.bfloat16)
    left = jnp.concatenate([win, ones], axis=1)
    for sub in range(rows // SUB):
        block = emb_ref[sub * SUB : (sub + 1) * SUB, :]
        total = None
        for lane in range(feats // LANES):
            piece = block[:, lane * LANES : (lane + 1) * LANES].astype(jnp.float32)
            total = piece * piece if total is None else total + piece * piece
        high = total.astype(jnp.bfloat16)
        low = (total - high.astype(jnp.float32)).astype(jnp.bfloat16)
        both = jnp.concatenate([block, high, low], axis=1)
        dots = lax.dot_general(left, both, NT, preferred_element_type=jnp.float32)
        start = pl.multiple_of(part * rows + sub * SUB, SUB)
        out_ref[0, :, pl.ds(start, SUB)] = dots[0:4, :]


def scan(embeddings, picked, winners, me, feat_size, first, count):
    cand_rows, feats = embeddings.shape
    chunk = cand_rows // feat_size
    rows = min(chunk, 2048)
    parts = chunk // rows
    return pl.pallas_call(
        functools.partial(scan_kernel, rows=rows, chunk=chunk, feats=feats, cand_rows=cand_rows),
        grid_spec=pltpu.PrefetchScalarGridSpec(
            num_scalar_prefetch=2,
            grid=(count, parts),
            in_specs=[
                pl.BlockSpec(picked.shape, lambda c, p, w, m: (0, 0, 0)),
                pl.BlockSpec((rows, feats), lambda c, p, w, m: (lax.bitwise_xor(m[0], first - c) * parts + p, 0)),
            ],
            out_specs=pl.BlockSpec((1, 4, chunk + LANES), lambda c, p, w, m: (c, 0, 0)),
            scratch_shapes=[pltpu.VMEM((LANES, feats), jnp.float32)],
        ),
        out_shape=jax.ShapeDtypeStruct((count, 4, chunk + LANES), jnp.float32),
        compiler_params=pltpu.CompilerParams(dimension_semantics=("arbitrary", "arbitrary")),
        name="scan",
    )(winners, me, picked, embeddings)


def update_kernel(*refs, feat_size, chunk):
    out_ref = refs[feat_size]
    total = refs[0][0]
    for src in range(1, feat_size):
        total = total + refs[src][0]
    table = total[:, chunk : chunk + LANES]
    gram = [[table[a : a + 1, b : b + 1] for b in range(STEPS)] for a in range(STEPS)]
    gains = total[STEPS : STEPS + 1, 0:chunk]
    coords = []
    winner_coords = [[None] * STEPS for _ in range(STEPS)]
    winner_gains = [gram[step][step] for step in range(STEPS)]
    for step in range(STEPS):
        scale = jnp.sqrt(jnp.maximum(winner_gains[step], 1.0))
        fresh = total[step : step + 1, 0:chunk]
        if step:
            proj = coords[0] * winner_coords[step][0]
            for prior in range(1, step):
                proj = proj + coords[prior] * winner_coords[step][prior]
            fresh = fresh - proj
        fresh = fresh / scale
        gains = gains - fresh * fresh
        coords.append(fresh)
        out_ref[step : step + 1, 0:chunk] = fresh
        out_ref[step : step + 1, chunk : chunk + LANES] = jnp.broadcast_to(jnp.max(gains, axis=1, keepdims=True), (1, LANES))
        for later in range(step + 1, STEPS):
            value = gram[later][step]
            for prior in range(step):
                value = value - winner_coords[later][prior] * winner_coords[step][prior]
            value = value / scale
            winner_coords[later][step] = value
            winner_gains[later] = winner_gains[later] - value * value
    out_ref[STEPS : STEPS + 1, 0:chunk] = gains
    out_ref[STEPS : STEPS + 1, chunk : chunk + LANES] = jnp.zeros((1, LANES), jnp.float32)


def update(parts, feat_size, chunk):
    return pl.pallas_call(
        functools.partial(update_kernel, feat_size=feat_size, chunk=chunk),
        out_shape=jax.ShapeDtypeStruct((4, chunk + LANES), jnp.float32),
        name="update",
    )(*parts)


def unpack_kernel(me_ref, *refs, feat_size, chunk):
    gains_ref, coords_ref, best_ref = refs[feat_size:]
    best = refs[0][:, chunk : chunk + LANES]
    for k in range(feat_size):
        start = pl.multiple_of(lax.bitwise_xor(me_ref[0], k) * chunk, chunk)
        coords_ref[:, pl.ds(start, chunk)] = refs[k][0:STEPS, 0:chunk]
        gains_ref[pl.ds(start, chunk)] = refs[k][STEPS : STEPS + 1, 0:chunk].reshape(chunk)
        best = jnp.maximum(best, refs[k][:, chunk : chunk + LANES])
    best_ref[...] = best


def unpack(pieces, me, feat_size, chunk):
    return pl.pallas_call(
        functools.partial(unpack_kernel, feat_size=feat_size, chunk=chunk),
        in_specs=[pl.BlockSpec(memory_space=pltpu.SMEM)] + [pl.BlockSpec(memory_space=pltpu.VMEM)] * feat_size,
        out_shape=(
            jax.ShapeDtypeStruct((feat_size * chunk,), jnp.float32),
            jax.ShapeDtypeStruct((STEPS, feat_size * chunk), jnp.float32),
            jax.ShapeDtypeStruct((4, LANES), jnp.float32),
        ),
        name="unpack",
    )(me, *pieces)


def swap(value, k, feat_size):
    return lax.ppermute(value, "feat", [(src, src ^ k) for src in range(feat_size)])


def per_device(embeddings, winners, *, feat_size):
    cand_rows = embeddings.shape[0]
    chunk = cand_rows // feat_size
    me = lax.axis_index("feat").astype(jnp.int32).reshape(1)
    picked = lax.all_gather(pick(embeddings, winners), "cand", axis=0, tiled=True)
    parts = []
    count = -(-feat_size // CALLS)
    first = feat_size - 1
    while first >= 0:
        here = min(count, first + 1)
        partial = scan(embeddings, picked, winners, me, feat_size, first, here)
        for c in range(here):
            piece = lax.slice_in_dim(partial, c, c + 1)
            k = first - c
            parts.append(swap(piece, k, feat_size) if k else piece)
        first -= here
    mine = update(parts, feat_size, chunk)
    pieces = [mine] + [swap(mine, k, feat_size) for k in range(1, feat_size)]
    gains, coords, best = unpack(pieces, me, feat_size, chunk)
    best = lax.pmax(best[0:STEPS, 0], "cand")
    return gains, coords, best


def solution(mesh):
    return jax.shard_map(
        functools.partial(per_device, feat_size=mesh.shape["feat"]),
        mesh=mesh,
        in_specs=(P("cand", "feat"), P()),
        out_specs=(P("cand"), P(None, "cand"), P()),
        check_vma=False,
    )
```
